8 devices in a mesh: dp: 2 (over z, y), tp: 4 (over x, core).
Axes of the slice: x: 2, y: 2, z: 1, core: 2. Of those that a mesh axis runs over, the one named last changes fastest.
Arguments:
- hidden_in: bfloat16 [256, 3072], P(('dp', 'tp')), parts along dimension 0
- attn_norm: bfloat16 [3072], replicated
- mlp_norm: bfloat16 [3072], replicated
- w_query: bfloat16 [3072, 24, 128], P(None, 'tp')
- w_key: bfloat16 [3072, 8, 128], replicated
- w_value: bfloat16 [3072, 8, 128], replicated
- w_out: bfloat16 [24, 128, 3072], P('tp')
- w_gate: bfloat16 [3072, 8192], P(None, 'tp')
- w_up: bfloat16 [3072, 8192], P(None, 'tp')
- w_down: bfloat16 [8192, 3072], P('tp')
Outputs:
- output 1: bfloat16 [256, 3072], P(('dp', 'tp')), parts along dimension 0
- output 2: bfloat16 [256, 8, 128], P('dp', 'tp'), parts along dimension 0
- output 3: bfloat16 [256, 8, 128], P('dp', 'tp'), parts along dimension 0
There are 2 independent parts. The reference program is written for one: setup_inputs(seed, part) draws one part's arguments, and reference() takes and returns one part's arrays. A program takes and returns all parts, laid end to end along the dimension named above; an argument that names none is the same for every part.
All inputs are finite; a program needn't handle non-finite values.
Results may differ from the reference program's by a relative error of at most 0.0144904.
Values are sent between devices in bfloat16 or wider.
A program may use at most 1 GiB of HBM per device.

```python
import jax
import jax.numpy as jnp
from jax import lax

TOKENS = 128
DIM = 3072
HEADS = 24
KV_HEADS = 8
HEAD = 128
FF = 8192
KV_SLOTS = 8
Q_BLOCK = min(128, TOKENS)


def setup_inputs(seed: int = 0, part: int = 0) -> dict:
    key_list = jax.random.split(jax.random.key(seed), 10)
    hidden_key = jax.random.fold_in(key_list[0], part)
    inner_width = HEADS * HEAD
    attn_gain = 1.5 * (TOKENS / 64) ** 0.25
    hidden = jax.random.normal(hidden_key, (TOKENS, DIM), jnp.float32)
    attn_norm = jax.random.uniform(key_list[1], (DIM,), jnp.float32, 0.5, 1.5)
    mlp_norm = jax.random.uniform(key_list[2], (DIM,), jnp.float32, 0.5, 1.5)
    w_query = jax.random.normal(key_list[3], (DIM, HEADS, HEAD), jnp.float32) * (1.5 * DIM ** -0.5)
    w_key = jax.random.normal(key_list[4], (DIM, KV_HEADS, HEAD), jnp.float32) * DIM ** -0.5
    w_value = jax.random.normal(key_list[5], (DIM, KV_HEADS, HEAD), jnp.float32) * DIM ** -0.5
    w_out = jax.random.normal(key_list[6], (HEADS, HEAD, DIM), jnp.float32) * (attn_gain * inner_width ** -0.5)
    w_gate = jax.random.normal(key_list[7], (DIM, FF), jnp.float32) * DIM ** -0.5
    w_up = jax.random.normal(key_list[8], (DIM, FF), jnp.float32) * DIM ** -0.5
    w_down = jax.random.normal(key_list[9], (FF, DIM), jnp.float32) * (1.5 * FF ** -0.5)
    return dict(hidden_in=hidden.astype(jnp.bfloat16), attn_norm=attn_norm.astype(jnp.bfloat16), mlp_norm=mlp_norm.astype(jnp.bfloat16), w_query=w_query.astype(jnp.bfloat16), w_key=w_key.astype(jnp.bfloat16), w_value=w_value.astype(jnp.bfloat16), w_out=w_out.astype(jnp.bfloat16), w_gate=w_gate.astype(jnp.bfloat16), w_up=w_up.astype(jnp.bfloat16), w_down=w_down.astype(jnp.bfloat16))


def rms_norm(rows_in, gain_vec):
    rows_f = rows_in.astype(jnp.float32)
    mean_sq = jnp.mean(rows_f * rows_f, axis=-1, keepdims=True)
    return (rows_f * lax.rsqrt(mean_sq + 1e-5) * gain_vec.astype(jnp.float32)).astype(jnp.bfloat16)


def apply_rope(heads_f, positions):
    head_dim = heads_f.shape[-1]
    half_dim = head_dim // 2
    inv_freq = 1.0 / (500000.0 ** (jnp.arange(half_dim).astype(jnp.float32) * (2.0 / head_dim)))
    angles = positions[:, None] * inv_freq[None, :]
    cosine = jnp.cos(angles)[:, None, :]
    sine_val = jnp.sin(angles)[:, None, :]
    first_half = heads_f[..., :half_dim]
    second_half = heads_f[..., half_dim:]
    return jnp.concatenate([first_half * cosine - second_half * sine_val, second_half * cosine + first_half * sine_val], axis=-1)


def reference(hidden_in, attn_norm, mlp_norm, w_query, w_key, w_value, w_out, w_gate, w_up, w_down):
    group_size = HEADS // KV_HEADS
    positions = jnp.arange(TOKENS).astype(jnp.float32)
    normed = rms_norm(hidden_in, attn_norm)
    q_proj = jnp.dot(normed, w_query.reshape(DIM, HEADS * HEAD), preferred_element_type=jnp.float32).reshape(TOKENS, HEADS, HEAD)
    k_proj = jnp.dot(normed, w_key.reshape(DIM, KV_HEADS * HEAD), preferred_element_type=jnp.float32).reshape(TOKENS, KV_HEADS, HEAD)
    v_proj = jnp.dot(normed, w_value.reshape(DIM, KV_HEADS * HEAD), preferred_element_type=jnp.float32).astype(jnp.bfloat16).reshape(TOKENS, KV_HEADS, HEAD)
    q_rot = apply_rope(q_proj, positions).astype(jnp.bfloat16)
    k_rot = apply_rope(k_proj, positions).astype(jnp.bfloat16)
    q_blocks = q_rot.reshape(TOKENS // Q_BLOCK, Q_BLOCK, KV_HEADS, group_size, HEAD)
    key_pos = jnp.arange(TOKENS)
    k_float = k_rot.astype(jnp.float32)
    v_float = v_proj.astype(jnp.float32)

    def one_block(block_args):
        q_block, block_idx = block_args
        scores = jnp.einsum("qgrd,kgd->grqk", q_block.astype(jnp.float32), k_float) * (HEAD ** -0.5)
        query_pos = block_idx * Q_BLOCK + jnp.arange(Q_BLOCK)
        visible = key_pos[None, :] <= query_pos[:, None]
        scores = jnp.where(visible, scores, -1e30)
        probs_bf = jax.nn.softmax(scores, axis=-1).astype(jnp.bfloat16)
        block_out = jnp.einsum("grqk,kgd->qgrd", probs_bf.astype(jnp.float32), v_float)
        return block_out.astype(jnp.bfloat16)

    attn_out = lax.map(one_block, (q_blocks, jnp.arange(TOKENS // Q_BLOCK)))
    attn_flat = attn_out.reshape(TOKENS, HEADS * HEAD)
    attn_res = jnp.dot(attn_flat, w_out.reshape(HEADS * HEAD, DIM), preferred_element_type=jnp.float32)
    resid_mid = (hidden_in.astype(jnp.float32) + attn_res).astype(jnp.bfloat16)
    normed_mlp = rms_norm(resid_mid, mlp_norm)
    gate_proj = jnp.dot(normed_mlp, w_gate, preferred_element_type=jnp.float32)
    up_proj = jnp.dot(normed_mlp, w_up, preferred_element_type=jnp.float32)
    mlp_act = (jax.nn.silu(gate_proj) * up_proj).astype(jnp.bfloat16)
    mlp_res = jnp.dot(mlp_act, w_down, preferred_element_type=jnp.float32)
    hidden_out = (resid_mid.astype(jnp.float32) + mlp_res).astype(jnp.bfloat16)
    k_cache = jnp.repeat(k_rot, KV_SLOTS // KV_HEADS, axis=1)
    v_cache = jnp.repeat(v_proj, KV_SLOTS // KV_HEADS, axis=1)
    return (hidden_out, k_cache, v_cache)
```

```python
import functools

import jax
import jax.numpy as jnp
import numpy as np
from jax import lax
from jax.experimental import pallas as pl
from jax.experimental.pallas import tpu as pltpu
from jax.sharding import PartitionSpec as P

T = 128
D = 3072
E = 128
R = 32
NH = 6
NKV = 2
F = 2048
CK = 512
NC = D // CK
EPS = 1e-5
F32 = jnp.float32
BF16 = jnp.bfloat16
MESH = pl.DeviceIdType.MESH

DIAG, PEER, CROSS, OWN = 0, 1, 2, 3


def rope_tables():
    half = E // 2
    inv_freq = (np.float32(1.0) / np.power(np.float32(500000.0), np.arange(half, dtype=np.float32) * np.float32(2.0 / E))).astype(np.float32)
    ang = np.arange(T, dtype=np.float32)[:, None] * inv_freq[None, :]
    cos = np.cos(ang.astype(np.float64)).astype(np.float32)
    sin = np.sin(ang.astype(np.float64)).astype(np.float32)
    return np.concatenate([cos, cos], 1), np.concatenate([-sin, sin], 1)


def dot(a, b):
    return lax.dot_general(a, b, (((1,), (0,)), ((), ())), preferred_element_type=F32)


def kernel(hid, an, mn, wq, wk, wv, wo, wg, wu, wd, cost, sint,
           out, kc, vc,
           hid_v, an_v, mn_v, wq_v, wk_v, wv_v, kvw, wo_v, wg_v, wu_v, wd_v, cos_v, sin_v,
           a1, a2, qkv, o_v, dsend, drecv, lsend, lrecv, ownf, crossf, mid, gacc, uacc, u_v, out_v, kc_v, vc_v,
           in_sem, wq_sem, gu_sem, wd_sem, out_sem, ag_s, ag_r, rs_s, rs_r):
    tp = lax.axis_index("tp")
    core = lax.rem(tp, 2)
    peer = tp + 1 - 2 * core
    cross = lax.rem(tp + 2, 4)
    diag = lax.rem(peer + 2, 4)
    devs = (diag, peer, cross, tp)
    rows = [pl.ds(pl.multiple_of(R * d, R), R) for d in devs]

    def start(copies):
        for cp in copies:
            cp.start()
        return copies

    small = start([pltpu.make_async_copy(s, d, in_sem.at[i]) for i, (s, d) in enumerate(
        [(hid, hid_v), (an, an_v), (mn, mn_v), (cost, cos_v), (sint, sin_v)])])
    kvc = start([pltpu.make_async_copy(wk.at[:, tp], wk_v, in_sem.at[5]),
                 pltpu.make_async_copy(wv.at[:, tp], wv_v, in_sem.at[6])])
    wqc = start([pltpu.make_async_copy(wq.at[:, pl.ds(CK * c, CK), :], wq_v.at[:, pl.ds(CK * c, CK), :], wq_sem.at[c])
                 for c in range(NC)])

    barrier = pltpu.get_barrier_semaphore()
    for d in (peer, cross):
        pl.semaphore_signal(barrier, inc=1, device_id={"tp": d}, device_id_type=MESH)
    pl.semaphore_wait(barrier, 2)

    def remote(src, dst, ss, rs, dev):
        return pltpu.make_async_remote_copy(src_ref=src, dst_ref=dst, send_sem=ss, recv_sem=rs,
                                            device_id={"tp": dev}, device_id_type=MESH)

    def ag_copies(ph, buf):
        blk = lambda c, p: buf.at[c, pl.ds(R * p, R), :]
        to_cross = [remote(blk(c, OWN), blk(c, CROSS), ag_s.at[ph, 0, c], ag_r.at[ph, 0, c], cross) for c in range(NC)]
        to_peer = [remote(blk(c, OWN), blk(c, PEER), ag_s.at[ph, 1, c], ag_r.at[ph, 1, c], peer) for c in range(NC)]
        fwd = [remote(blk(c, CROSS), blk(c, DIAG), ag_s.at[ph, 2, c], ag_r.at[ph, 2, c], peer) for c in range(NC)]
        return to_cross, to_peer, fwd

    def norm_send(x, gain_v, buf, copies):
        ss = None
        for c in range(NC):
            sq = x(c) * x(c)
            ss = sq if ss is None else ss + sq
        inv = lax.rsqrt(jnp.sum(ss, axis=-1, keepdims=True) * (1.0 / D) + EPS)
        gain = gain_v[...].astype(F32)
        to_cross, to_peer, _ = copies
        for c in range(NC):
            n = CK // 128
            g = jnp.concatenate([gain[c * n + j:c * n + j + 1, :] for j in range(n)], axis=1)
            buf[c, R * OWN:R * OWN + R, :] = (x(c) * inv * g).astype(BF16)
            to_cross[c].start()
            to_peer[c].start()

    for cp in small[:2]:
        cp.wait()
    ag1 = ag_copies(0, a1)
    norm_send(lambda c: hid_v[:, CK * c:CK * c + CK].astype(F32), an_v, a1, ag1)

    i0 = lax.broadcasted_iota(jnp.int32, (256, 256), 0)
    i1 = lax.broadcasted_iota(jnp.int32, (256, 256), 1)
    src_row = jnp.where(i0 < 128, 2 * i0, 2 * i0 - 255)
    perm = jnp.where(src_row == i1, 1.0, 0.0).astype(BF16)
    for cp in kvc:
        cp.wait()

    def split(b, _):
        dst = pl.ds(pl.multiple_of(128 * b, 128), 128)
        blk = jnp.concatenate([wk_v[dst].reshape(256, E), wv_v[dst].reshape(256, E)], axis=1)
        r = dot(perm, blk).astype(BF16)
        kvw[0, dst, :] = r[:128, :128]
        kvw[1, dst, :] = r[128:, :128]
        kvw[2, dst, :] = r[:128, 128:]
        kvw[3, dst, :] = r[128:, 128:]
        return 0

    lax.fori_loop(0, 2 * D // 256, split, 0)

    woc = pltpu.make_async_copy(wo, wo_v, in_sem.at[7])
    woc.start()
    guc = []
    for c in range(NC):
        guc.append(start([pltpu.make_async_copy(s.at[pl.ds(CK * c, CK), :], d.at[pl.ds(CK * c, CK), :], gu_sem.at[i, c])
                          for i, (s, d) in enumerate([(wg, wg_v), (wu, wu_v)])]))
    wdc = start([pltpu.make_async_copy(wd.at[pl.ds(512 * c, 512), :], wd_v.at[pl.ds(512 * c, 512), :], wd_sem.at[c])
                 for c in range(F // 512)])

    def gather_loop(copies, compute):
        to_cross, to_peer, fwd = copies
        for c in range(NC + 1):
            if c < NC:
                to_cross[c].wait_recv()
                fwd[c].start()
            if c >= 1:
                to_peer[c - 1].wait_recv()
                fwd[c - 1].wait_recv()
                compute(c - 1)
        for c in range(NC):
            to_cross[c].wait_send()
            to_peer[c].wait_send()
            fwd[c].wait_send()

    def qkv_chunk(c):
        wqc[c].wait()
        lhs = a1[c]
        for h in range(NH + 2 * NKV):
            w = wq_v[h, CK * c:CK * c + CK, :] if h < NH else kvw[h - NH, CK * c:CK * c + CK, :]
            p = dot(lhs, w)
            qkv[h] = p if c == 0 else qkv[h] + p

    gather_loop(ag1, qkv_chunk)

    for cp in small[3:]:
        cp.wait()
    cos = jnp.concatenate([cos_v[r, :] for r in rows], axis=0)
    sin = jnp.concatenate([sin_v[r, :] for r in rows], axis=0)

    def token_of(i):
        b = i // R
        base = jnp.where(b == DIAG, diag, jnp.where(b == PEER, peer, jnp.where(b == CROSS, cross, tp)))
        return base * R + i % R

    visible = (token_of(lax.broadcasted_iota(jnp.int32, (T, T), 1))
               <= token_of(lax.broadcasted_iota(jnp.int32, (T, T), 0)))

    def rope(x):
        return (x * cos + pltpu.roll(x, E // 2, 1) * sin).astype(BF16)

    for g in range(NKV):
        k = rope(qkv[NH + g])
        v = qkv[NH + NKV + g].astype(BF16)
        for p in range(4):
            kc_v[g, rows[p], :] = k[R * p:R * p + R]
            vc_v[g, rows[p], :] = v[R * p:R * p + R]
        for r in range(NH // NKV):
            h = g * (NH // NKV) + r
            q = rope(qkv[h])
            s = lax.dot_general(q, k, (((1,), (1,)), ((), ())), preferred_element_type=F32) * (E ** -0.5)
            s = jnp.where(visible, s, -1e30)
            e = jnp.exp(s - jnp.max(s, axis=-1, keepdims=True))
            pr = (e / jnp.sum(e, axis=-1, keepdims=True)).astype(BF16)
            o_v[:, E * h:E * h + E] = dot(pr, v).astype(BF16)
    cache_out = start([pltpu.make_async_copy(kc_v, kc, out_sem.at[NC]), pltpu.make_async_copy(vc_v, vc, out_sem.at[NC + 1])])

    def reduce_phase(ph, product):
        d2d = [remote(dsend.at[ph, n], drecv.at[ph, n], rs_s.at[ph, 0, n], rs_r.at[ph, 0, n], peer) for n in range(NC)]
        link = [remote(lsend.at[ph, n], lrecv.at[ph, n], rs_s.at[ph, 1, n], rs_r.at[ph, 1, n], cross) for n in range(NC)]
        for n in range(NC + 1):
            if n < NC:
                p = product(n)
                dsend[ph, n] = p[:2 * R].astype(BF16)
                crossf[n] = p[R * CROSS:R * CROSS + R]
                ownf[n] = p[R * OWN:R * OWN + R]
                d2d[n].start()
            if n >= 1:
                d2d[n - 1].wait_recv()
                lsend[ph, n - 1] = (crossf[n - 1] + drecv[ph, n - 1, :R].astype(F32)).astype(BF16)
                link[n - 1].start()
        return d2d, link

    def total(ph, n):
        return ownf[n] + drecv[ph, n, R:].astype(F32) + lrecv[ph, n].astype(F32)

    woc.wait()
    d2d, link = reduce_phase(0, lambda n: dot(o_v[...], wo_v[:, CK * n:CK * n + CK]))
    for n in range(NC):
        link[n].wait_recv()
        mid[n] = (hid_v[:, CK * n:CK * n + CK].astype(F32) + total(0, n)).astype(BF16)
    small[2].wait()
    ag2 = ag_copies(1, a2)
    norm_send(lambda c: mid[c].astype(F32), mn_v, a2, ag2)
    for n in range(NC):
        d2d[n].wait_send()
        link[n].wait_send()

    NB = 512

    def gu_chunk(c):
        for cp in guc[c]:
            cp.wait()

        def block(b, _):
            col = pl.ds(pl.multiple_of(NB * b, NB), NB)
            pg = dot(a2[c], wg_v[CK * c:CK * c + CK, col])
            pu = dot(a2[c], wu_v[CK * c:CK * c + CK, col])
            if c == 0:
                gacc[:, col] = pg
                uacc[:, col] = pu
            elif c < NC - 1:
                gacc[:, col] += pg
                uacc[:, col] += pu
            else:
                gate = gacc[:, col] + pg
                up = uacc[:, col] + pu
                u_v[:, col] = (gate * jax.nn.sigmoid(gate) * up).astype(BF16)
            return 0

        lax.fori_loop(0, F // NB, block, 0)

    gather_loop(ag2, gu_chunk)

    for cp in wdc:
        cp.wait()
    d2d, link = reduce_phase(1, lambda n: dot(u_v[...], wd_v[:, CK * n:CK * n + CK]))
    outs = []
    for n in range(NC):
        link[n].wait_recv()
        out_v[n] = (mid[n].astype(F32) + total(1, n)).astype(BF16)
        cp = pltpu.make_async_copy(out_v.at[n], out.at[:, pl.ds(CK * n, CK)], out_sem.at[n])
        cp.start()
        outs.append(cp)
    for n in range(NC):
        d2d[n].wait_send()
        link[n].wait_send()
    for cp in outs + cache_out:
        cp.wait()


def solution(mesh):
    def local_layer(hidden_in, attn_norm, mlp_norm, w_query, w_key, w_value, w_out, w_gate, w_up, w_down):
        cos, sin = rope_tables()
        any_spec = pl.BlockSpec(memory_space=pl.ANY)
        vm = pltpu.VMEM
        dma = pltpu.SemaphoreType.DMA
        out, kc, vc = pl.pallas_call(
            kernel,
            name="layer",
            out_shape=[jax.ShapeDtypeStruct((R, D), BF16),
                       jax.ShapeDtypeStruct((NKV, T, E), BF16),
                       jax.ShapeDtypeStruct((NKV, T, E), BF16)],
            in_specs=[any_spec] * 12,
            out_specs=[any_spec] * 3,
            scratch_shapes=[
                vm((R, D), BF16), vm((D // 128, 128), BF16), vm((D // 128, 128), BF16),
                vm((NH, D, E), BF16), vm((D, 2, E), BF16), vm((D, 2, E), BF16), vm((2 * NKV, D, E), BF16),
                vm((NH * E, D), BF16), vm((D, F), BF16), vm((D, F), BF16), vm((F, D), BF16),
                vm((T, E), F32), vm((T, E), F32),
                vm((NC, T, CK), BF16), vm((NC, T, CK), BF16),
                vm((NH + 2 * NKV, T, E), F32), vm((T, NH * E), BF16),
                vm((2, NC, 2 * R, CK), BF16), vm((2, NC, 2 * R, CK), BF16),
                vm((2, NC, R, CK), BF16), vm((2, NC, R, CK), BF16),
                vm((NC, R, CK), F32), vm((NC, R, CK), F32), vm((NC, R, CK), BF16),
                vm((T, F), F32), vm((T, F), F32), vm((T, F), BF16),
                vm((NC, R, CK), BF16), vm((NKV, T, E), BF16), vm((NKV, T, E), BF16),
                dma((8,)), dma((NC,)), dma((2, NC)), dma((F // 512,)), dma((NC + 2,)),
                dma((2, 3, NC)), dma((2, 3, NC)), dma((2, 2, NC)), dma((2, 2, NC)),
            ],
            compiler_params=pltpu.CompilerParams(collective_id=0, has_side_effects=True, vmem_limit_bytes=67043328),
        )(hidden_in, attn_norm.reshape(D // 128, 128), mlp_norm.reshape(D // 128, 128),
          jnp.transpose(w_query, (1, 0, 2)), w_key.reshape(D, 4, 2, E), w_value.reshape(D, 4, 2, E),
          w_out.reshape(NH * E, D), w_gate, w_up, w_down, jnp.asarray(cos), jnp.asarray(sin))
        return out, jnp.transpose(kc, (1, 0, 2)), jnp.transpose(vc, (1, 0, 2))

    row_spec = P(("dp", "tp"), None)
    cache_spec = P("dp", "tp", None)
    return jax.shard_map(local_layer, mesh=mesh, in_specs=(row_spec, P(), P(), P(None, "tp", None), P(), P(), P("tp", None, None), P(None, "tp"), P(None, "tp"), P("tp", None)), out_specs=(row_spec, cache_spec, cache_spec), check_vma=False)
```

```python
import functools

import jax
import jax.numpy as jnp
import numpy as np
from jax import lax
from jax.experimental import pallas as pl
from jax.experimental.pallas import tpu as pltpu
from jax.sharding import PartitionSpec as P

T = 128
D = 3072
E = 128
R = 32
NH = 6
NKV = 2
F = 2048
CK = 512
NC = D // CK
EPS = 1e-5
F32 = jnp.float32
BF16 = jnp.bfloat16
MESH = pl.DeviceIdType.MESH
scope = jax.named_scope

SUB = 256
AG1 = ((0, 1), (1, 1), (2, 2), (4, 2), (6, 2), (8, 2), (10, 1), (11, 1))
AG2 = ((0, 1), (1, 1), (2, 2), (4, 2), (6, 2), (8, 2), (10, 2))
DEPTH = 3

DIAG, CROSS, PEER, OWN = 0, 1, 2, 3


def rope_tables():
    half = E // 2
    inv_freq = (np.float32(1.0) / np.power(np.float32(500000.0), np.arange(half, dtype=np.float32) * np.float32(2.0 / E))).astype(np.float32)
    ang = np.arange(T, dtype=np.float32)[:, None] * inv_freq[None, :]
    cos = np.cos(ang.astype(np.float64)).astype(np.float32)
    sin = np.sin(ang.astype(np.float64)).astype(np.float32)
    return np.concatenate([cos, cos], 1), np.concatenate([-sin, sin], 1)


def dot(a, b):
    return lax.dot_general(a, b, (((1,), (0,)), ((), ())), preferred_element_type=F32)


def kernel(hid, an, mn, wq, wk, wv, wo, wg, wu, wd, cost, sint,
           out, kc, vc,
           hid_v, an_v, mn_v, wq_v, wk_v, wv_v, kvw, wo_v, wg_v, wu_v, wd_v, cos_v, sin_v,
           a1, a2, qkv, o_v, dsend, drecv, lsend, lrecv, ownf, crossf, mid, gacc, uacc, u_v, k_v, v_v,
           in_sem, wq_sem, gu_sem, wd_sem, ag_s, ag_r, rs_s, rs_r):
    tp = lax.axis_index("tp")
    core = lax.rem(tp, 2)
    peer = tp + 1 - 2 * core
    cross = lax.rem(tp + 2, 4)
    diag = lax.rem(peer + 2, 4)
    devs = (diag, cross, peer, tp)
    rows = [pl.ds(pl.multiple_of(R * d, R), R) for d in devs]

    def start(copies):
        for cp in copies:
            cp.start()
        return copies

    small = start([pltpu.make_async_copy(s, d, in_sem.at[i]) for i, (s, d) in enumerate(
        [(hid, hid_v), (an, an_v), (mn, mn_v), (cost, cos_v), (sint, sin_v)])])
    kvc = start([pltpu.make_async_copy(wk.at[:, tp], wk_v, in_sem.at[5]),
                 pltpu.make_async_copy(wv.at[:, tp], wv_v, in_sem.at[6])])

    barrier = pltpu.get_barrier_semaphore()
    for d in (peer, cross):
        pl.semaphore_signal(barrier, inc=1, device_id={"tp": d}, device_id_type=MESH)

    wqc = start([pltpu.make_async_copy(wq.at[:, pl.ds(SUB * a, SUB * n), :], wq_v.at[:, pl.ds(SUB * a, SUB * n), :], wq_sem.at[c])
                 for c, (a, n) in enumerate(AG1)])
    woc = pltpu.make_async_copy(wo, wo_v, in_sem.at[7])
    woc.start()
    with scope("barrier"):
        pl.semaphore_wait(barrier, 2)

    def remote(src, dst, ss, rs, dev):
        return pltpu.make_async_remote_copy(src_ref=src, dst_ref=dst, send_sem=ss, recv_sem=rs,
                                            device_id={"tp": dev}, device_id_type=MESH)

    def ag_copies(ph, buf, plan):
        def copies(i, p, q, dev):
            return [remote(buf.at[pl.ds(a, n), pl.ds(R * p, R), :], buf.at[pl.ds(a, n), pl.ds(R * q, R), :],
                           ag_s.at[ph, i, c], ag_r.at[ph, i, c], dev) for c, (a, n) in enumerate(plan)]
        return copies(0, OWN, CROSS, cross), copies(1, OWN, PEER, peer), copies(2, CROSS, DIAG, peer)

    def norm_send(x, gain_v, buf, plan, copies):
        ss = None
        for i in range(D // SUB):
            sq = x(i) * x(i)
            ss = sq if ss is None else ss + sq
        inv = lax.rsqrt(jnp.sum(ss, axis=-1, keepdims=True) * (1.0 / D) + EPS)
        gain = gain_v[...].astype(F32)
        to_cross, to_peer, _ = copies

        def send(c):
            if c < DEPTH:
                to_cross[c].start()
            to_peer[c].start()

        for c, (a, n) in enumerate(plan):
            for i in range(a, a + n):
                g = jnp.concatenate([gain[2 * i:2 * i + 1, :], gain[2 * i + 1:2 * i + 2, :]], axis=1)
                buf[i, R * OWN:R * OWN + R, :] = (x(i) * inv * g).astype(BF16)
            if c >= 1:
                send(c - 1)
        send(len(plan) - 1)

    ag1 = ag_copies(0, a1, AG1)
    with scope("hidwait"):
        for cp in small[:2]:
            cp.wait()
    with scope("norm1"):
        norm_send(lambda i: hid_v[:, SUB * i:SUB * i + SUB].astype(F32), an_v, a1, AG1, ag1)

    i0 = lax.broadcasted_iota(jnp.int32, (256, 256), 0)
    i1 = lax.broadcasted_iota(jnp.int32, (256, 256), 1)
    perm = jnp.where(jnp.where(i0 < 128, 2 * i0, 2 * i0 - 255) == i1, 1.0, 0.0).astype(BF16)
    with scope("kvwait"):
        for cp in kvc:
            cp.wait()

    def split(b, _):
        dst = pl.ds(pl.multiple_of(128 * b, 128), 128)
        blk = jnp.concatenate([wk_v[dst].reshape(256, E), wv_v[dst].reshape(256, E)], axis=1)
        r = dot(perm, blk).astype(BF16)
        kvw[0, dst, :] = r[:128, :128]
        kvw[1, dst, :] = r[128:, :128]
        kvw[2, dst, :] = r[:128, 128:]
        kvw[3, dst, :] = r[128:, 128:]
        return 0

    with scope("split"):
        lax.fori_loop(0, D // 128, split, 0, unroll=8)

    guc = []
    for c, (a, n) in enumerate(AG2):
        guc.append(start([pltpu.make_async_copy(s.at[pl.ds(SUB * a, SUB * n), :], d.at[pl.ds(SUB * a, SUB * n), :], gu_sem.at[i, c])
                          for i, (s, d) in enumerate([(wg, wg_v), (wu, wu_v)])]))
    wdc = start([pltpu.make_async_copy(wd.at[pl.ds(512 * c, 512), :], wd_v.at[pl.ds(512 * c, 512), :], wd_sem.at[c])
                 for c in range(F // 512)])

    def gather_loop(name, copies, compute):
        to_cross, to_peer, fwd = copies
        n = len(fwd)
        for c in range(n + 1):
            if c < n:
                with scope(f"{name}_x{c}"):
                    to_cross[c].wait_recv()
                fwd[c].start()
                if c + DEPTH < n:
                    with scope(f"{name}_s{c}"):
                        to_cross[c].wait_send()
                    to_cross[c + DEPTH].start()
            if c >= 1:
                with scope(f"{name}_f{c - 1}"):
                    to_peer[c - 1].wait_recv()
                    fwd[c - 1].wait_recv()
                with scope(f"{name}_c{c - 1}"):
                    compute(c - 1)
        with scope(f"{name}_ws"):
            for c in range(n):
                if c + DEPTH >= n:
                    to_cross[c].wait_send()
                to_peer[c].wait_send()
                fwd[c].wait_send()

    def lhs_of(buf, a, n):
        return buf[a] if n == 1 else jnp.concatenate([buf[a + i] for i in range(n)], axis=1)

    def qkv_chunk(c):
        a, n = AG1[c]
        wqc[c].wait()
        lhs = lhs_of(a1, a, n)
        for h in range(NH + 2 * NKV):
            w = wq_v[h, SUB * a:SUB * (a + n), :] if h < NH else kvw[h - NH, SUB * a:SUB * (a + n), :]
            p = dot(lhs, w)
            qkv[h] = p if c == 0 else qkv[h] + p

    gather_loop("ag1", ag1, qkv_chunk)

    for cp in small[3:]:
        cp.wait()
    cos = jnp.concatenate([cos_v[r, :] for r in rows], axis=0)
    sin = jnp.concatenate([sin_v[r, :] for r in rows], axis=0)

    def token_of(i):
        b = i // R
        base = jnp.where(b == DIAG, diag, jnp.where(b == CROSS, cross, jnp.where(b == PEER, peer, tp)))
        return base * R + i % R

    visible = (token_of(lax.broadcasted_iota(jnp.int32, (T, T), 1))
               <= token_of(lax.broadcasted_iota(jnp.int32, (T, T), 0)))

    def rope(x, half=None):
        cs, sn = (cos, sin) if half is None else (cos[half], sin[half])
        return (x * cs + pltpu.roll(x, E // 2, 1) * sn).astype(BF16)

    def keys_values():
        for g in range(NKV):
            k = rope(qkv[NH + g])
            v = qkv[NH + NKV + g].astype(BF16)
            for p in range(4):
                k_v[g, rows[p], :] = k[R * p:R * p + R]
                v_v[g, rows[p], :] = v[R * p:R * p + R]
            qkv[NH + g] = k.astype(F32)

    def attend(half, g):
        k = qkv[NH + g].astype(BF16)
        v = qkv[NH + NKV + g].astype(BF16)
        for r in range(NH // NKV):
            h = g * (NH // NKV) + r
            q = rope(qkv[h, half], half)
            s = lax.dot_general(q, k, (((1,), (1,)), ((), ())), preferred_element_type=F32) * (E ** -0.5)
            s = jnp.where(visible[half], s, -1e30)
            e = jnp.exp(s - jnp.max(s, axis=-1, keepdims=True))
            pr = (e * (1.0 / jnp.sum(e, axis=-1, keepdims=True))).astype(BF16)
            o_v[half, E * h:E * h + E] = dot(pr, v).astype(BF16)

    far, near = slice(0, 2 * R), slice(2 * R, 4 * R)

    def rs_copies(ph):
        row = lambda buf, n, i: buf.at[ph, n, pl.ds(R * i, R), :]
        dfar = [remote(row(dsend, n, 0), row(drecv, n, 0), rs_s.at[ph, 0, n], rs_r.at[ph, 0, n], peer) for n in range(NC)]
        dnear = [remote(row(dsend, n, 1), row(drecv, n, 1), rs_s.at[ph, 1, n], rs_r.at[ph, 1, n], peer) for n in range(NC)]
        link = [remote(lsend.at[ph, n], lrecv.at[ph, n], rs_s.at[ph, 2, n], rs_r.at[ph, 2, n], cross) for n in range(NC)]
        return dfar, dnear, link

    def send_sum(ph, copies, n):
        dfar, _, link = copies
        with scope(f"rs{ph}_d{n}"):
            dfar[n].wait_recv()
        lsend[ph, n] = (crossf[n] + drecv[ph, n, :R].astype(F32)).astype(BF16)
        link[n].start()

    def put_far(ph, copies, n, p):
        dsend[ph, n, :R] = p[:R].astype(BF16)
        crossf[n] = p[R:2 * R]
        copies[0][n].start()

    def put_near(ph, copies, n, p):
        dsend[ph, n, R:] = p[:R].astype(BF16)
        ownf[n] = p[R:2 * R]
        copies[1][n].start()

    def total(ph, copies, n):
        with scope(f"rs{ph}_n{n}"):
            copies[1][n].wait_recv()
        part = ownf[n] + drecv[ph, n, R:].astype(F32)
        with scope(f"rs{ph}_x{n}"):
            copies[2][n].wait_recv()
        return part + lrecv[ph, n].astype(F32)

    def drain(copies):
        for group in copies:
            for cp in group:
                cp.wait_send()

    rs0 = rs_copies(0)
    with scope("attnA"):
        keys_values()
        for g in range(NKV):
            attend(far, g)
    with scope("wowait"):
        woc.wait()
    for n in range(NC):
        with scope(f"rs0_p{n}"):
            put_far(0, rs0, n, dot(o_v[far, :], wo_v[:, CK * n:CK * n + CK]))
        if n >= 4:
            send_sum(0, rs0, n - 4)
    with scope("attnB0"):
        attend(near, 0)
    send_sum(0, rs0, 2)
    send_sum(0, rs0, 3)
    with scope("attnB1"):
        attend(near, 1)
    send_sum(0, rs0, 4)
    send_sum(0, rs0, 5)
    for n in range(NC):
        with scope(f"rs0_q{n}"):
            put_near(0, rs0, n, dot(o_v[near, :], wo_v[:, CK * n:CK * n + CK]))

    with scope("cache"):
        inter = jnp.where(i1 == i0 // 2 + 128 * (i0 % 2), 1.0, 0.0).astype(BF16)
        kv = jnp.concatenate([jnp.concatenate([k_v[0], k_v[1]], axis=0), jnp.concatenate([v_v[0], v_v[1]], axis=0)], axis=1)
        kv = dot(inter, kv).astype(BF16)
        kc[...] = kv[:, :E]
        vc[...] = kv[:, E:]

    for n in range(NC):
        t = total(0, rs0, n)
        m = (hid_v[:, CK * n:CK * n + CK].astype(F32) + t).astype(BF16)
        mid[2 * n] = m[:, :SUB]
        mid[2 * n + 1] = m[:, SUB:]
    small[2].wait()
    ag2 = ag_copies(1, a2, AG2)
    with scope("norm2"):
        norm_send(lambda i: mid[i].astype(F32), mn_v, a2, AG2, ag2)
    drain(rs0)

    NB = 512

    def gu_chunk(c):
        a, n = AG2[c]
        for cp in guc[c]:
            cp.wait()
        lhs = lhs_of(a2, a, n)
        k = slice(SUB * a, SUB * (a + n))
        for b in range(F // NB):
            col = slice(NB * b, NB * b + NB)
            pg = dot(lhs, wg_v[k, col])
            pu = dot(lhs, wu_v[k, col])
            if c == 0:
                gacc[:, col] = pg
                uacc[:, col] = pu
            elif c < len(AG2) - 1:
                gacc[:, col] += pg
                uacc[:, col] += pu
            else:
                gate = gacc[:, col] + pg
                up = uacc[:, col] + pu
                u_v[:, col] = (gate * jax.nn.sigmoid(gate) * up).astype(BF16)

    gather_loop("ag2", ag2, gu_chunk)

    with scope("wdwait"):
        for cp in wdc:
            cp.wait()
    rs1 = rs_copies(1)
    LA = 2
    for n in range(NC + LA):
        if n < NC:
            with scope(f"rs1_p{n}"):
                p = dot(u_v[...], wd_v[:, CK * n:CK * n + CK])
                put_far(1, rs1, n, p[far])
                put_near(1, rs1, n, p[near])
        if n >= LA:
            send_sum(1, rs1, n - LA)
    for n in range(NC):
        t = total(1, rs1, n)
        m = jnp.concatenate([mid[2 * n], mid[2 * n + 1]], axis=1).astype(F32)
        out[:, CK * n:CK * n + CK] = (m + t).astype(BF16)
    drain(rs1)


def store_kernel(a, b, c, oa, ob, oc, sem):
    copies = [pltpu.make_async_copy(s, d, sem.at[i]) for i, (s, d) in enumerate([(a, oa), (b, ob), (c, oc)])]
    for cp in copies:
        cp.start()
    for cp in copies:
        cp.wait()


def solution(mesh):
    def local_layer(hidden_in, attn_norm, mlp_norm, w_query, w_key, w_value, w_out, w_gate, w_up, w_down):
        cos, sin = rope_tables()
        any_spec = pl.BlockSpec(memory_space=pl.ANY)
        vm = pltpu.VMEM
        dma = pltpu.SemaphoreType.DMA
        vm_spec = pl.BlockSpec(memory_space=pltpu.VMEM)
        shapes = [(R, D), (NKV * T, E), (NKV * T, E)]
        res = pl.pallas_call(
            kernel,
            name="layer",
            out_shape=[vm(s, BF16) for s in shapes],
            in_specs=[any_spec] * 12,
            out_specs=[vm_spec] * 3,
            scratch_shapes=[
                vm((R, D), BF16), vm((D // 128, 128), BF16), vm((D // 128, 128), BF16),
                vm((NH, D, E), BF16), vm((D, 2, E), BF16), vm((D, 2, E), BF16), vm((2 * NKV, D, E), BF16),
                vm((NH * E, D), BF16), vm((D, F), BF16), vm((D, F), BF16), vm((F, D), BF16),
                vm((T, E), F32), vm((T, E), F32),
                vm((D // SUB, T, SUB), BF16), vm((D // SUB, T, SUB), BF16),
                vm((NH + 2 * NKV, T, E), F32), vm((T, NH * E), BF16),
                vm((2, NC, 2 * R, CK), BF16), vm((2, NC, 2 * R, CK), BF16),
                vm((2, NC, R, CK), BF16), vm((2, NC, R, CK), BF16),
                vm((NC, R, CK), F32), vm((NC, R, CK), F32), vm((D // SUB, R, SUB), BF16),
                vm((T, F), F32), vm((T, F), F32), vm((T, F), BF16),
                vm((NKV, T, E), BF16), vm((NKV, T, E), BF16),
                dma((8,)), dma((len(AG1),)), dma((2, len(AG2))), dma((F // 512,)),
                dma((2, 3, len(AG1))), dma((2, 3, len(AG1))), dma((2, 3, NC)), dma((2, 3, NC)),
            ],
            compiler_params=pltpu.CompilerParams(collective_id=0, has_side_effects=True, vmem_limit_bytes=64500000),
        )(hidden_in, attn_norm.reshape(D // 128, 128), mlp_norm.reshape(D // 128, 128),
          jnp.transpose(w_query, (1, 0, 2)), w_key.reshape(D, 4, 2, E), w_value.reshape(D, 4, 2, E),
          w_out.reshape(NH * E, D), w_gate, w_up, w_down, jnp.asarray(cos), jnp.asarray(sin))
        out, kc, vc = pl.pallas_call(
            store_kernel,
            name="store",
            out_shape=[jax.ShapeDtypeStruct(s, BF16) for s in shapes],
            in_specs=[vm_spec] * 3,
            out_specs=[any_spec] * 3,
            scratch_shapes=[dma((3,))],
            compiler_params=pltpu.CompilerParams(vmem_limit_bytes=1 << 20),
        )(*res)
        return out, kc.reshape(T, NKV, E), vc.reshape(T, NKV, E)

    row_spec = P(("dp", "tp"), None)
    cache_spec = P("dp", "tp", None)
    return jax.shard_map(local_layer, mesh=mesh, in_specs=(row_spec, P(), P(), P(None, "tp", None), P(), P(), P("tp", None, None), P(None, "tp"), P(None, "tp"), P("tp", None)), out_specs=(row_spec, cache_spec, cache_spec), check_vma=False)
```
